32 devices in a mesh: dp: 8 (over y, x, core), tensor: 4 (over z).
Axes of the slice: x: 2, y: 2, z: 4, core: 2. Of those that a mesh axis runs over, the one named last changes fastest.
Arguments:
- tokens: bfloat16 [4096, 2048], P(('dp', 'tensor')), may hold values from -6 to 6
- cotangent: bfloat16 [4096, 2048], P(('dp', 'tensor')), may hold values from -6 to 6
- ln_gain: bfloat16 [2, 2048], P(None, 'dp'), may hold values from 0.5 to 1.5
- ln_shift: bfloat16 [2, 2048], P(None, 'dp'), may hold values from -1.75 to 1.75
- w_qkv: bfloat16 [2, 2048, 3, 2048], P(None, 'dp', None, 'tensor'), may hold values from -1 to 1
- b_qkv: bfloat16 [2, 3, 2048], P(None, None, ('tensor', 'dp')), may hold values from -3 to 3
- w_out: bfloat16 [2, 2048, 2048], P(None, 'tensor', 'dp'), may hold values from -1.5 to 1.5
- w_one: bfloat16 [2, 2048, 8192], P(None, 'dp', 'tensor'), may hold values from -0.125 to 0.125
- b_one: bfloat16 [2, 8192], P(None, ('tensor', 'dp')), may hold values from -3 to 3
- w_two: bfloat16 [2, 8192, 2048], P(None, 'tensor', 'dp'), may hold values from -0.0625 to 0.0625
- out_bias: bfloat16 [2, 2048], P(None, 'dp'), may hold values from -3 to 3
Outputs:
- outputs: bfloat16 [4096, 2048], P(('dp', 'tensor'))
- input_grad: float32 [4096, 2048], P(('dp', 'tensor'))
- grad_gain: float32 [2, 2048], P(None, ('dp', 'tensor'))
- grad_shift: float32 [2, 2048], P(None, ('dp', 'tensor'))
- grad_qkv: float32 [2, 2048, 3, 2048], P(None, 'dp', None, 'tensor')
- grad_b_qkv: float32 [2, 3, 2048], P(None, None, ('tensor', 'dp'))
- grad_out: float32 [2, 2048, 2048], P(None, 'tensor', 'dp')
- grad_one: float32 [2, 2048, 8192], P(None, 'dp', 'tensor')
- grad_b_one: float32 [2, 8192], P(None, ('tensor', 'dp'))
- grad_two: float32 [2, 8192, 2048], P(None, 'tensor', 'dp')
- grad_out_bias: float32 [2, 2048], P(None, ('dp', 'tensor'))
The draws below stay inside these ranges and needn't reach their ends.
All inputs are finite; a program needn't handle non-finite values.
Results may differ from the reference program's by a relative error of at most 0.019.
Values may be sent and summed in bfloat16 or wider, within the bound.
A program may use at most 256 MiB of HBM per device.

```python
import jax
import jax.numpy as jnp
from jax import lax

D = 2048
HEADS = 32
HEAD = 64
ROT = 32
FF = 8192
SEQ_LEN = 512
LAYERS = 2
SEQ_DEV = 1
TOKENS = 4096
N_TENSOR = 4


def draw_w_qkv(key, part):
    base_key = jax.random.fold_in(key, 0)
    weight_scale = D ** (-0.5)
    base = jnp.clip(jax.random.normal(base_key, (LAYERS, D, 3, D), jnp.float32), -6.0, 6.0) * weight_scale
    return jnp.clip(base, -1.0, 1.0).astype(jnp.bfloat16)


def with_spikes(values, rng, source, target, shards_of, factor):
    owner, partner = [(jnp.arange(values.shape[position]) // (values.shape[position] // shards_of)).reshape([-1 if axis == position else 1 for axis in range(values.ndim)]) for position in (source, target)]
    chosen = jax.random.permutation(rng, shards_of)[partner]
    strong = (owner == chosen) | (owner == (partner + shards_of // 2) % shards_of)
    return jnp.where(strong, factor * values, values)


def block_scale(key, extent, cuts, low, top_value):
    def one(position, shards_of):
        steps = jax.random.uniform(jax.random.fold_in(jax.random.fold_in(key, 6), position), (shards_of,), jnp.float32, low / len(cuts), top_value / len(cuts))
        return jnp.repeat(jnp.exp(steps), extent[position] // shards_of).reshape((-1,) + (1,) * (len(extent) - position - 1))

    factor_of = one(*cuts[0])
    for cut in cuts[1:]:
        factor_of = factor_of * one(*cut)
    return factor_of


def scatter_about(key, extent, scale, bound, shards=(), kind=jnp.bfloat16):
    result = scale * jax.random.normal(key, extent, jnp.float32)
    if shards:
        result = result * block_scale(key, extent, shards, -0.22, 0.18)
    return jnp.clip(result, -bound, bound).astype(kind)


def noise_with(stream_key, extent, scale, reach, cuts, heavy, held_as=jnp.bfloat16):
    result = scale * jax.random.normal(stream_key, extent, jnp.float32)
    if cuts:
        result = result * block_scale(stream_key, extent, cuts, -0.22, 0.18)
    return jnp.clip(with_spikes(result, jax.random.fold_in(stream_key, 3), *heavy), -reach, reach).astype(held_as)


def setup_inputs(seed: int = 0) -> dict:
    seeds = jax.random.split(jax.random.key(seed), 12)
    tokens = scatter_about(seeds[0], (TOKENS, D), 1.0, 6.0, ((0, 32),))
    cotangent = noise_with(seeds[1], (TOKENS, D), 1.0, 6.0, ((0, 32),), (0, 1, 32, 2.75))
    ln_gain = jnp.clip(1.0 + 0.1 * jax.random.normal(seeds[2], (LAYERS, D), jnp.float32), 0.5, 1.5).astype(jnp.bfloat16)
    ln_shift = scatter_about(seeds[3], (LAYERS, D), 0.3, 1.75, ((1, 8),))
    w_qkv = draw_w_qkv(jax.random.fold_in(seeds[11], 71), 0)
    b_qkv = scatter_about(seeds[5], (LAYERS, 3, D), 0.5, 3.0, ((2, 32),))
    w_out = scatter_about(seeds[6], (LAYERS, D, D), (D // 128) ** -0.5, 1.5, ((1, 4), (2, 8)))
    w_one = scatter_about(seeds[7], (LAYERS, D, FF), D ** -0.5, 0.125, ((1, 8), (2, 4)))
    b_one = scatter_about(seeds[8], (LAYERS, FF), 0.5, 3.0, ((1, 32),))
    w_two = scatter_about(seeds[9], (LAYERS, FF, D), FF ** -0.5, 0.0625, ((1, 4), (2, 8)))
    out_bias = scatter_about(seeds[10], (LAYERS, D), 0.5, 3.0, ((1, 8),))
    return dict(tokens=tokens, cotangent=cotangent, ln_gain=ln_gain, ln_shift=ln_shift, w_qkv=w_qkv, b_qkv=b_qkv, w_out=w_out, w_one=w_one, b_one=b_one, w_two=w_two, out_bias=out_bias)


EPSILON = 1e-05
GELU_SCALE = 0.7978845608028654
GELU_CUBIC = 0.044715

def matmul(left, right):
    return jnp.dot(left, right, preferred_element_type=jnp.float32)

def batched(form, left, right):
    return jnp.einsum(form, left.astype(jnp.float32), right.astype(jnp.float32))

def rotary_tables(length, rotary):
    half_width = rotary // 2
    exponent = jnp.arange(half_width, dtype=jnp.float32) * (2.0 / rotary)
    frequency = 10000.0 ** (-exponent)
    angles = jnp.arange(length, dtype=jnp.float32)[:, None] * frequency[None, :]
    return (jnp.cos(angles), jnp.sin(angles))

def rotate(field, cosine, sine_table):
    half_width = cosine.shape[-1]
    front_half = field[..., :half_width]
    back_half = field[..., half_width:2 * half_width]
    passive = field[..., 2 * half_width:]
    cos_rows = cosine[:, None, :]
    sin_rows = sine_table[:, None, :]
    return jnp.concatenate([front_half * cos_rows - back_half * sin_rows, back_half * cos_rows + front_half * sin_rows, passive], axis=-1)

def layer_norm(stream, norm_gain, norm_shift):
    average = lax.optimization_barrier(jnp.mean(stream, -1, keepdims=True))
    centred = stream - average
    variance = lax.optimization_barrier(jnp.mean(centred * centred, -1, keepdims=True))
    inv_scale = lax.rsqrt(variance + EPSILON)
    unit_rows = centred * inv_scale
    return (unit_rows * norm_gain + norm_shift, unit_rows, inv_scale)

def norm_backward(grad_normed, unit_rows, inv_scale, norm_gain):
    scaled = grad_normed * norm_gain
    return inv_scale * (scaled - lax.optimization_barrier(jnp.mean(scaled, -1, keepdims=True)) - unit_rows * lax.optimization_barrier(jnp.mean(scaled * unit_rows, -1, keepdims=True)))

def gelu_parts(preact):
    inside = GELU_SCALE * (preact + GELU_CUBIC * preact * preact * preact)
    tangent = jnp.tanh(inside)
    active = 0.5 * preact * (1.0 + tangent)
    gelu_slope = 0.5 * (1.0 + tangent) + 0.5 * preact * (1.0 - tangent * tangent) * GELU_SCALE * (1.0 + 3.0 * GELU_CUBIC * preact * preact)
    return (active, gelu_slope)

def project_heads(normed, w_qkv, b_qkv, seq_count):
    model_width = w_qkv.shape[0]
    local_width = w_qkv.shape[2]
    merged = matmul(normed, w_qkv.reshape(model_width, 3 * local_width)) + b_qkv.astype(jnp.float32).reshape(3 * local_width)
    merged = merged.reshape(seq_count, SEQ_LEN, 3, local_width // HEAD, HEAD)
    cosine, sine_table = rotary_tables(SEQ_LEN, ROT)
    queries = rotate(merged[:, :, 0], cosine, sine_table).astype(jnp.bfloat16)
    key_rows = rotate(merged[:, :, 1], cosine, sine_table).astype(jnp.bfloat16)
    values = merged[:, :, 2].astype(jnp.bfloat16)
    return (queries, key_rows, values)

def attention_weights(queries, key_rows, log_total):
    scores = batched('bqhd,bkhd->bhqk', queries, key_rows) * HEAD ** (-0.5)
    positions = jnp.arange(queries.shape[1])
    allowed = positions[:, None] >= positions[None, :]
    scores = jnp.where(allowed, scores, -1e+30)
    if log_total is None:
        largest = lax.optimization_barrier(jnp.max(scores, -1, keepdims=True))
        log_total = largest[..., 0] + jnp.log(lax.optimization_barrier(jnp.sum(jnp.exp(scores - largest), -1)))
    return (jnp.exp(scores - log_total[..., None]), log_total)

def forward_branches(normed, layer_params, seq_count):
    w_qkv, b_qkv, w_out, w_one, b_one, w_two = layer_params[3:]
    local_width = w_qkv.shape[2]
    queries, key_rows, values = project_heads(normed, w_qkv, b_qkv, seq_count)
    attend, log_total = attention_weights(queries, key_rows, None)
    mixture = batched('bhqk,bkhd->bqhd', attend.astype(jnp.bfloat16), values).astype(jnp.bfloat16)
    mixture = mixture.reshape(seq_count * SEQ_LEN, local_width)
    preact = matmul(normed, w_one) + b_one.astype(jnp.float32)
    active, gelu_slope = gelu_parts(preact)
    branch_total = matmul(mixture, w_out) + matmul(active.astype(jnp.bfloat16), w_two)
    return (branch_total, log_total)

def backward_branches(normed, down_rows, log_total, layer_params, seq_count):
    w_qkv, b_qkv, w_out, w_one, b_one, w_two = layer_params[3:]
    model_width = w_qkv.shape[0]
    local_width = w_qkv.shape[2]
    queries, key_rows, values = project_heads(normed, w_qkv, b_qkv, seq_count)
    attend, unused_total = attention_weights(queries, key_rows, log_total)
    attend_half = attend.astype(jnp.bfloat16)
    mixture = batched('bhqk,bkhd->bqhd', attend_half, values).astype(jnp.bfloat16)
    mixture = mixture.reshape(seq_count * SEQ_LEN, local_width)
    preact = matmul(normed, w_one) + b_one.astype(jnp.float32)
    active, gelu_slope = gelu_parts(preact)
    grad_two = matmul(active.astype(jnp.bfloat16).T, down_rows)
    grad_out = matmul(mixture.T, down_rows)
    grad_preact = matmul(down_rows, w_two.T) * gelu_slope
    grad_b_one = lax.optimization_barrier(jnp.sum(grad_preact, 0))
    preact_half = grad_preact.astype(jnp.bfloat16)
    grad_one = matmul(normed.T, preact_half)
    grad_mixture = matmul(down_rows, w_out.T).astype(jnp.bfloat16)
    grad_mixture = grad_mixture.reshape(seq_count, SEQ_LEN, local_width // HEAD, HEAD)
    grad_attend = batched('bqhd,bkhd->bhqk', grad_mixture, values)
    grad_value = batched('bhqk,bqhd->bkhd', attend_half, grad_mixture)
    grad_score = attend * (grad_attend - lax.optimization_barrier(jnp.sum(attend * grad_attend, -1, keepdims=True))) * HEAD ** (-0.5)
    grad_score = grad_score.astype(jnp.bfloat16)
    grad_query = batched('bhqk,bkhd->bqhd', grad_score, key_rows)
    grad_key = batched('bhqk,bqhd->bkhd', grad_score, queries)
    cosine, sine_table = rotary_tables(SEQ_LEN, ROT)
    grad_query = rotate(grad_query, cosine, -sine_table)
    grad_key = rotate(grad_key, cosine, -sine_table)
    grad_merged = jnp.stack([grad_query, grad_key, grad_value], axis=2).reshape(seq_count * SEQ_LEN, 3 * local_width)
    grad_b_qkv = lax.optimization_barrier(jnp.sum(grad_merged, 0)).reshape(3, local_width)
    merged_half = grad_merged.astype(jnp.bfloat16)
    grad_qkv = matmul(normed.T, merged_half).reshape(model_width, 3, local_width)
    grad_normed = matmul(merged_half, w_qkv.reshape(model_width, 3 * local_width).T) + matmul(preact_half, w_one.T)
    return (grad_normed, (grad_qkv, grad_b_qkv, grad_out, grad_one, grad_b_one, grad_two))

def group_params(layer_params, group):
    width_part = D // N_TENSOR
    hidden_part = FF // N_TENSOR
    col_lo = group * width_part
    ff_lo = group * hidden_part
    w_qkv, b_qkv, w_out, w_one, b_one, w_two = layer_params[3:]
    return layer_params[:3] + (w_qkv[:, :, col_lo:col_lo + width_part], b_qkv[:, col_lo:col_lo + width_part], w_out[col_lo:col_lo + width_part, :], w_one[:, ff_lo:ff_lo + hidden_part], b_one[ff_lo:ff_lo + hidden_part], w_two[ff_lo:ff_lo + hidden_part, :])

def rounded_term(partial_sum):
    held = lax.optimization_barrier(partial_sum.astype(jnp.bfloat16))
    return held.astype(jnp.float32)

def reference(tokens, cotangent, ln_gain, ln_shift, w_qkv, b_qkv, w_out, w_one, b_one, w_two, out_bias):
    block_rows = SEQ_DEV * SEQ_LEN
    blocks = TOKENS // block_rows
    head_part = HEADS // N_TENSOR

    def params_of(layer_index):
        return (ln_gain[layer_index].astype(jnp.float32), ln_shift[layer_index].astype(jnp.float32), out_bias[layer_index].astype(jnp.float32), w_qkv[layer_index], b_qkv[layer_index], w_out[layer_index], w_one[layer_index], b_one[layer_index], w_two[layer_index])

    def block_step(totals, pieces):
        token_block, cotangent_block = pieces
        stream = token_block.astype(jnp.float32)
        inputs = []
        log_totals = []
        for layer_index in range(LAYERS):
            layer_params = params_of(layer_index)
            normed, unit_rows, inv_scale = layer_norm(stream, layer_params[0], layer_params[1])
            normed_half = normed.astype(jnp.bfloat16)
            branch_sum = jnp.zeros((block_rows, D), jnp.float32)
            group_totals = []
            for group in range(N_TENSOR):
                branch_total, log_total = forward_branches(normed_half, group_params(layer_params, group), SEQ_DEV)
                branch_sum = branch_sum + rounded_term(branch_total)
                group_totals.append(log_total)
            inputs.append(stream)
            log_totals.append(jnp.concatenate(group_totals, axis=1))
            stream = stream + branch_sum + layer_params[2]
        block_out = stream.astype(jnp.bfloat16)
        residual_grad = cotangent_block.astype(jnp.float32)
        per_layer = [None] * LAYERS
        for layer_index in reversed(range(LAYERS)):
            layer_params = params_of(layer_index)
            normed, unit_rows, inv_scale = layer_norm(inputs[layer_index], layer_params[0], layer_params[1])
            normed_half = normed.astype(jnp.bfloat16)
            down_half = residual_grad.astype(jnp.bfloat16)
            grad_normed = jnp.zeros((block_rows, D), jnp.float32)
            group_terms = []
            for group in range(N_TENSOR):
                group_total = log_totals[layer_index][:, group * head_part:(group + 1) * head_part]
                grad_part, weight_terms = backward_branches(normed_half, down_half, group_total, group_params(layer_params, group), SEQ_DEV)
                grad_normed = grad_normed + rounded_term(grad_part)
                group_terms.append(weight_terms)
            joined_axes = (2, 1, 0, 1, 0, 0)
            weight_terms = tuple((jnp.concatenate([group_terms[group][member] for group in range(N_TENSOR)], axis=joined_axes[member]) for member in range(6)))
            norm_terms = (lax.optimization_barrier(jnp.sum(grad_normed * unit_rows, 0)), lax.optimization_barrier(jnp.sum(grad_normed, 0)), lax.optimization_barrier(jnp.sum(residual_grad, 0)))
            residual_grad = residual_grad + norm_backward(grad_normed, unit_rows, inv_scale, layer_params[0])
            per_layer[layer_index] = norm_terms + weight_terms
        stacked = tuple((jnp.stack([per_layer[layer_index][member] for layer_index in range(LAYERS)]) for member in range(9)))
        totals = tuple((running + fresh for running, fresh in zip(totals, stacked)))
        return (totals, (block_out, residual_grad))
    initial = (jnp.zeros((LAYERS, D), jnp.float32), jnp.zeros((LAYERS, D), jnp.float32), jnp.zeros((LAYERS, D), jnp.float32), jnp.zeros((LAYERS, D, 3, D), jnp.float32), jnp.zeros((LAYERS, 3, D), jnp.float32), jnp.zeros((LAYERS, D, D), jnp.float32), jnp.zeros((LAYERS, D, FF), jnp.float32), jnp.zeros((LAYERS, FF), jnp.float32), jnp.zeros((LAYERS, FF, D), jnp.float32))
    totals, (block_outs, block_grads) = lax.scan(block_step, initial, (tokens.reshape(blocks, block_rows, D), cotangent.reshape(blocks, block_rows, D)))
    return (block_outs.reshape(TOKENS, D), block_grads.reshape(TOKENS, D), totals[0], totals[1], totals[3], totals[4], totals[5], totals[6], totals[7], totals[8], totals[2])
```

```python
import functools
import math

import jax
import jax.numpy as jnp
import numpy as np
from jax import lax
from jax.experimental import pallas as pl
from jax.experimental.pallas import tpu as pltpu
from jax.sharding import Mesh
from jax.sharding import PartitionSpec as P

HEAD = 64
ROT = 32
SEQ_LEN = 512
LANES = 128

EPSILON = 1e-05
GELU_SCALE = 0.7978845608028654
GELU_CUBIC = 0.044715
F32 = jnp.float32
BF16 = jnp.bfloat16


def dot(left, right, contract):
    return lax.dot_general(left, right, (contract, ((), ())), preferred_element_type=F32)


def matmul(left, right):
    return dot(left, right, ((1,), (0,)))


def rotary_lanes(length):
    half = ROT // 2
    exponent = jnp.arange(half, dtype=F32) * (2.0 / ROT)
    frequency = 10000.0 ** (-exponent)
    angles = jnp.arange(length, dtype=F32)[:, None] * frequency[None, :]
    cosine, sine = jnp.cos(angles), jnp.sin(angles)
    rest = HEAD - ROT
    ones, zeros = jnp.ones((length, rest), F32), jnp.zeros((length, rest), F32)
    blank = jnp.zeros_like(sine)
    straight = jnp.concatenate([cosine, cosine, ones], 1)
    ahead = jnp.concatenate([-sine, blank, zeros], 1)
    behind = jnp.concatenate([blank, sine, zeros], 1)
    return tuple(jnp.concatenate([table] * (LANES // HEAD), 1) for table in (straight, ahead, behind))


def turn(field, straight, ahead, behind, sign):
    half = ROT // 2
    forward = pltpu.roll(field, LANES - half, 1)
    backward = pltpu.roll(field, half, 1)
    if sign > 0:
        return field * straight + forward * ahead + backward * behind
    return field * straight - forward * ahead - backward * behind


def causal_probabilities(query, keys, first_row):
    scores = dot(query, keys, ((1,), (1,))) * HEAD ** (-0.5)
    rows = first_row + lax.broadcasted_iota(jnp.int32, scores.shape, 0)
    columns = lax.broadcasted_iota(jnp.int32, scores.shape, 1)
    scores = jnp.where(rows >= columns, scores, -1e30)
    largest = jnp.max(scores, -1, keepdims=True)
    grown = jnp.exp(scores - largest)
    return grown / jnp.sum(grown, -1, keepdims=True)


def forward_kernel(q_ref, k_ref, v_ref, bq_ref, bk_ref, bv_ref, c_ref, a_ref, b_ref, rq_ref, rk_ref, rv_ref, mix_ref):
    tables = (c_ref[...], a_ref[...], b_ref[...])
    query = turn(q_ref[...] + bq_ref[...], *tables, 1).astype(BF16)
    keys = turn(k_ref[...] + bk_ref[...], *tables, 1).astype(BF16)
    values = (v_ref[...] + bv_ref[...]).astype(BF16)
    rq_ref[...] = query
    rk_ref[...] = keys
    rv_ref[...] = values
    length = query.shape[0]
    step = length // 2
    lane = lax.broadcasted_iota(jnp.int32, (step, LANES), 1)
    for block in range(2):
        reach = (block + 1) * step
        rows = slice(block * step, reach)
        result = None
        for head in range(LANES // HEAD):
            own = (lane // HEAD) == head
            part = jnp.where(own, query[rows], jnp.zeros((), BF16))
            attend = causal_probabilities(part, keys[:reach], block * step)
            mixed = matmul(attend.astype(BF16), values[:reach])
            result = mixed if result is None else jnp.where(own, mixed, result)
        mix_ref[rows, :] = result.astype(BF16)


def attention_forward(merged, bias, tables, width):
    rows = merged.shape[0]
    sequences, pairs = rows // SEQ_LEN, width // LANES
    block = (SEQ_LEN, LANES)

    def part(which):
        return pl.BlockSpec(block, lambda s, h: (s, which * pairs + h))

    def bias_part(which):
        return pl.BlockSpec((1, LANES), lambda s, h: (0, which * pairs + h))

    whole = pl.BlockSpec(block, lambda s, h: (0, 0))
    out = pl.BlockSpec(block, lambda s, h: (s, h))
    half = jax.ShapeDtypeStruct((rows, width), BF16)
    return pl.pallas_call(
        forward_kernel,
        grid=(sequences, pairs),
        in_specs=[part(0), part(1), part(2), bias_part(0), bias_part(1), bias_part(2), whole, whole, whole],
        out_specs=[out] * 4,
        out_shape=[half] * 4,
        cost_estimate=pl.CostEstimate(
            flops=4 * rows * SEQ_LEN * width, bytes_accessed=rows * width * 20, transcendentals=rows * SEQ_LEN * width // HEAD
        ),
        name="attention_forward",
    )(merged, merged, merged, bias, bias, bias, *tables)


def backward_kernel(q_ref, k_ref, v_ref, g_ref, c_ref, a_ref, b_ref, out_ref, sum_ref, dq_ref, dk_ref, dv_ref):
    stage = pl.program_id(2)

    @pl.when(stage == 0)
    def _():
        query, keys, values, grad = q_ref[...], k_ref[...], v_ref[...], g_ref[...]
        length = query.shape[0]
        step = length // 2
        lane = lax.broadcasted_iota(jnp.int32, (step, LANES), 1)
        zero = jnp.zeros((), BF16)
        for block in range(2):
            reach = (block + 1) * step
            rows = slice(block * step, reach)
            lane_all = lax.broadcasted_iota(jnp.int32, (reach, LANES), 1)
            dq = dk = dv = None
            for head in range(LANES // HEAD):
                own = (lane // HEAD) == head
                own_all = (lane_all // HEAD) == head
                q_part = jnp.where(own, query[rows], zero)
                g_part = jnp.where(own, grad[rows], zero)
                attend = causal_probabilities(q_part, keys[:reach], block * step)
                grad_attend = dot(g_part, values[:reach], ((1,), (1,)))
                centre = jnp.sum(attend * grad_attend, -1, keepdims=True)
                grad_score = (attend * (grad_attend - centre) * HEAD ** (-0.5)).astype(BF16)
                new_dq = matmul(grad_score, keys[:reach])
                new_dk = dot(grad_score, q_part, ((0,), (0,)))
                new_dv = dot(attend.astype(BF16), g_part, ((0,), (0,)))
                if head == 0:
                    dq, dk, dv = new_dq, new_dk, new_dv
                else:
                    dq = jnp.where(own, new_dq, dq)
                    dk = dk + new_dk
                    dv = dv + new_dv
            dq_ref[rows, :] = dq
            if block == 0:
                dk_ref[:reach, :] = dk
                dv_ref[:reach, :] = dv
            else:
                dk_ref[:step, :] += dk[:step]
                dk_ref[step:, :] = dk[step:]
                dv_ref[:step, :] += dv[:step]
                dv_ref[step:, :] = dv[step:]

    def put(field):
        out_ref[...] = field.astype(BF16)
        sum_ref[...] = jnp.broadcast_to(jnp.sum(field, 0, keepdims=True), sum_ref.shape)

    @pl.when(stage == 0)
    def _():
        put(turn(dq_ref[...], c_ref[...], a_ref[...], b_ref[...], -1))

    @pl.when(stage == 1)
    def _():
        put(turn(dk_ref[...], c_ref[...], a_ref[...], b_ref[...], -1))

    @pl.when(stage == 2)
    def _():
        put(dv_ref[...])


def attention_backward(query, keys, values, grad, tables):
    rows, width = query.shape
    sequences, pairs = rows // SEQ_LEN, width // LANES
    block = (SEQ_LEN, LANES)
    same = pl.BlockSpec(block, lambda s, h, i: (s, h))
    whole = pl.BlockSpec(block, lambda s, h, i: (0, 0))
    return pl.pallas_call(
        backward_kernel,
        grid=(sequences, pairs, 3),
        in_specs=[same] * 4 + [whole] * 3,
        out_specs=[
            pl.BlockSpec(block, lambda s, h, i: (s, i * pairs + h)),
            pl.BlockSpec((8, LANES), lambda s, h, i: (s, i * pairs + h)),
        ],
        out_shape=[
            jax.ShapeDtypeStruct((rows, 3 * width), BF16),
            jax.ShapeDtypeStruct((8 * sequences, 3 * width), F32),
        ],
        scratch_shapes=[pltpu.VMEM(block, F32)] * 3,
        cost_estimate=pl.CostEstimate(
            flops=10 * rows * SEQ_LEN * width, bytes_accessed=rows * width * 14, transcendentals=rows * SEQ_LEN * width // HEAD
        ),
        name="attention_backward",
    )(query, keys, values, grad, *tables)


def normalize(stream):
    average = jnp.mean(stream, -1, keepdims=True)
    centred = stream - average
    variance = jnp.mean(centred * centred, -1, keepdims=True)
    inv_scale = lax.rsqrt(variance + EPSILON)
    return centred * inv_scale, inv_scale


def norm_backward(grad_normed, unit_rows, inv_scale, norm_gain):
    scaled = grad_normed * norm_gain
    return inv_scale * (
        scaled
        - jnp.mean(scaled, -1, keepdims=True)
        - unit_rows * jnp.mean(scaled * unit_rows, -1, keepdims=True)
    )


def gelu_active(preact):
    inside = GELU_SCALE * (preact + GELU_CUBIC * preact * preact * preact)
    return 0.5 * preact * (1.0 + jnp.tanh(inside))


def gelu_slope(preact):
    inside = GELU_SCALE * (preact + GELU_CUBIC * preact * preact * preact)
    tangent = jnp.tanh(inside)
    return 0.5 * (1.0 + tangent) + 0.5 * preact * (1.0 - tangent * tangent) * GELU_SCALE * (
        1.0 + 3.0 * GELU_CUBIC * preact * preact
    )


def on_device(chips, n_tensor, tokens, cotangent, ln_gain, ln_shift, w_qkv, b_qkv, w_out, w_one, b_one, w_two, out_bias):
    layers, block_d = w_qkv.shape[0], w_qkv.shape[1]
    model = block_d * 2 * chips
    width = w_qkv.shape[3] // 2
    hidden = w_one.shape[2] // 2
    rows = tokens.shape[0]
    chip, core, tensor = lax.axis_index("chip"), lax.axis_index("core"), lax.axis_index("tensor")
    bits = [1 << i for i in range(int(math.log2(chips)))]

    def to_chip(value, offset):
        return lax.ppermute(value, "chip", [(i, i ^ offset) for i in range(chips)])

    def to_core(value):
        return lax.ppermute(value, "core", [(0, 1), (1, 0)])

    def pick(first, second):
        return jnp.where(core == 0, first, second)

    def relative(blocks):
        for bit in bits:
            flip = (chip & bit) != 0
            blocks = [jnp.where(flip, blocks[j ^ bit], blocks[j]) for j in range(chips)]
        return blocks

    def reorder_columns(value):
        span = 2 * block_d
        return jnp.concatenate(relative([value[:, j * span : (j + 1) * span] for j in range(chips)]), 1)

    def core_half(value, axis, which):
        span = value.shape[axis] // 2
        return lax.dynamic_slice_in_dim(value, which * span, span, axis)

    def gather_chips(halves):
        blocks = {(0, 0): halves[0], (0, 1): halves[1]}
        if chips == 4:
            blocks[1, 0] = to_chip(halves[0], 1)
            blocks[2, 1] = to_chip(halves[1], 2)
            blocks[1, 1] = to_chip(halves[1], 1)
            blocks[2, 0] = to_chip(halves[0], 2)
            blocks[3, 0] = to_chip(blocks[1, 0], 2)
            blocks[3, 1] = to_chip(blocks[2, 1], 1)
        else:
            for bit in bits:
                for j in range(bit):
                    for s in range(2):
                        blocks[j | bit, s] = to_chip(blocks[j, s], bit)
        return [blocks[j, s] for j in range(chips) for s in range(2)]

    def scatter_chips(make):
        if chips == 4:
            far0 = to_chip(make(3, 0).astype(BF16), 2)
            far1 = to_chip(make(3, 1).astype(BF16), 1)
            x1 = to_chip(make(1, 1).astype(BF16), 1)
            y0 = to_chip(make(2, 0).astype(BF16), 2)
            x0 = to_chip((make(1, 0) + far0.astype(F32)).astype(BF16), 1)
            y1 = to_chip((make(2, 1) + far1.astype(F32)).astype(BF16), 2)
            return [
                (make(0, 0) + x0.astype(F32) + y0.astype(F32)).astype(BF16),
                (make(0, 1) + x1.astype(F32) + y1.astype(F32)).astype(BF16),
            ]
        parts = {(j, s): make(j, s) for j in range(chips) for s in range(2)}
        for bit in reversed(bits):
            for j in range(bit):
                for s in range(2):
                    arrived = to_chip(parts[j | bit, s].astype(BF16), bit)
                    parts[j, s] = parts[j, s] + arrived.astype(F32)
        return [parts[0, s].astype(BF16) for s in range(2)]

    def finish(sums, axis):
        mine = pick(sums[0], sums[1])
        other = to_core(pick(sums[1], sums[0]))
        return jnp.concatenate([pick(mine, other), pick(other, mine)], axis).astype(F32)

    packed = jnp.concatenate(
        [value.reshape(-1) for value in (ln_gain, ln_shift, out_bias, b_qkv, b_one)]
    )
    everyone = lax.all_gather(packed, ("chip", "core"), axis=0)
    count = layers * block_d
    norm_part = everyone[:, : 3 * count].reshape(chips, 2, 3, layers, block_d)
    norm_part = jnp.stack(relative([norm_part[j] for j in range(chips)]))
    norm_part = norm_part.transpose(2, 3, 0, 1, 4).reshape(3, layers, 1, model).astype(F32)
    gains, shifts, biases = norm_part[0], norm_part[1], norm_part[2]
    group_bias = core_half(everyone[:, 3 * count :], 0, core)
    piece = layers * 3 * b_qkv.shape[2]
    bias_qkv = group_bias[:, :piece].reshape(chips, layers, 3, b_qkv.shape[2])
    bias_qkv = bias_qkv.transpose(1, 2, 0, 3).reshape(layers, 1, 3 * width).astype(F32)
    bias_one = group_bias[:, piece:].reshape(chips, layers, b_one.shape[1])
    bias_one = bias_one.transpose(1, 0, 2).reshape(layers, 1, hidden).astype(F32)

    def exchange(mine, other):
        arrived = to_core(other)
        return [pick(mine, arrived), pick(arrived, mine)]

    def first_weights(layer):
        def half(which):
            return jnp.concatenate(
                [core_half(w_qkv[layer], 2, which).reshape(block_d, 3 * width), core_half(w_one[layer], 1, which)], 1
            )

        return jnp.concatenate(gather_chips(exchange(half(core), half(1 - core))), 0)

    def second_weights(layer):
        def half(which):
            return jnp.concatenate([core_half(w_out[layer], 0, which), core_half(w_two[layer], 0, which)], 0)

        return jnp.concatenate(gather_chips(exchange(half(core), half(1 - core))), 1)

    def gather_rows(value):
        return lax.all_gather(value.astype(BF16), ("core", "tensor"), axis=0, tiled=True)

    def scatter_rows(left, right, contract):
        sent = to_core(dot(core_half(left, 0, 1 - core), right, contract).astype(BF16))
        total = dot(core_half(left, 0, core), right, contract) + sent.astype(F32)
        return lax.psum_scatter(total.astype(BF16), "tensor", scatter_dimension=0, tiled=True).astype(F32)

    tables = rotary_lanes(SEQ_LEN)
    stream = reorder_columns(tokens.astype(F32))
    residual_grad = reorder_columns(cotangent.astype(F32))
    first = [first_weights(layer) for layer in range(layers)]
    second = [second_weights(layer) for layer in range(layers)]

    kept = []
    for layer in range(layers):
        unit_rows, inv_scale = normalize(stream)
        normed = gather_rows(unit_rows * gains[layer] + shifts[layer])
        raw = matmul(normed, first[layer])
        query, keys, values, mixture = attention_forward(raw, bias_qkv[layer], tables, width)
        preact = raw[:, 3 * width :] + bias_one[layer]
        active = gelu_active(preact).astype(BF16)
        both = jnp.concatenate([mixture, active], 1)
        kept.append((unit_rows, inv_scale, normed, query, keys, values, raw, both))
        stream = stream + scatter_rows(both, second[layer], ((1,), (0,))) + biases[layer]
    outputs = reorder_columns(stream).astype(BF16)

    large = [None] * layers
    small = [None] * layers
    for layer in reversed(range(layers)):
        unit_rows, inv_scale, normed, query, keys, values, raw, both = kept[layer]
        down = gather_rows(residual_grad)
        back = dot(down, second[layer], ((1,), (1,)))
        preact = raw[:, 3 * width :] + bias_one[layer]
        grad_preact = back[:, width:] * gelu_slope(preact)
        sum_one = jnp.sum(grad_preact, 0)
        preact_half = grad_preact.astype(BF16)

        def columns(value, j, s):
            start = (2 * j + s) * block_d
            return value[:, start : start + block_d]

        grad_one = scatter_chips(lambda j, s: dot(columns(normed, j, s), preact_half, ((0,), (0,))))
        grad_second = scatter_chips(lambda j, s: dot(both, columns(down, j, s), ((0,), (0,))))
        merged_half, sums = attention_backward(query, keys, values, back[:, :width].astype(BF16), tables)
        sum_qkv = jnp.sum(sums.reshape(-1, 8, 3 * width)[:, 0], 0)
        grad_qkv = scatter_chips(lambda j, s: dot(columns(normed, j, s), merged_half, ((0,), (0,))))
        grad_normed = scatter_rows(
            jnp.concatenate([merged_half, preact_half], 1), first[layer], ((1,), (1,))
        )
        small[layer] = (
            jnp.sum(grad_normed * unit_rows, 0),
            jnp.sum(grad_normed, 0),
            jnp.sum(residual_grad, 0),
            sum_qkv,
            sum_one,
        )
        grad_second = finish([value.reshape(1, width + hidden, block_d) for value in grad_second], 0)
        large[layer] = (
            finish([value.reshape(block_d, 3, width) for value in grad_qkv], 2),
            grad_second[:, :width].reshape(2 * width, block_d),
            finish(grad_one, 1),
            grad_second[:, width:].reshape(2 * hidden, block_d),
        )
        residual_grad = residual_grad + norm_backward(grad_normed, unit_rows, inv_scale, gains[layer])
    input_grad = reorder_columns(residual_grad)

    norm_sums = jnp.stack([jnp.stack([small[layer][i] for layer in range(layers)]) for i in range(3)])
    norm_sums = norm_sums.reshape(3 * layers, model)
    norm_sums = reorder_columns(norm_sums)
    qkv_sums = jnp.stack([small[layer][3] for layer in range(layers)])
    one_sums = jnp.stack([small[layer][4] for layer in range(layers)])
    bundle = jnp.concatenate([norm_sums.reshape(-1), qkv_sums.reshape(-1), one_sums.reshape(-1)])
    bundles = lax.all_gather(bundle, ("chip", "core", "tensor"), axis=0)
    cut = norm_sums.size
    device = chip * 2 + core
    norm_total = jnp.sum(bundles[:, :cut], 0).reshape(3, layers, model)
    span = model // (2 * chips * n_tensor)
    norm_total = lax.dynamic_slice_in_dim(norm_total, (device * n_tensor + tensor) * span, span, 2)
    local = bundles[:, cut:].reshape(chips, 2, n_tensor, -1)
    local = lax.dynamic_index_in_dim(jnp.sum(local, 0), tensor, 1, keepdims=False)
    local = lax.dynamic_index_in_dim(local, device // chips, 0, keepdims=False)
    cut = qkv_sums.size
    place = lax.rem(device, chips)
    span = width // chips
    grad_b_qkv = lax.dynamic_slice_in_dim(local[:cut].reshape(layers, 3, width), place * span, span, 2)
    span = hidden // chips
    grad_b_one = lax.dynamic_slice_in_dim(local[cut:].reshape(layers, hidden), place * span, span, 1)

    stacked = [jnp.stack([large[layer][member] for layer in range(layers)]) for member in range(4)]
    return (
        outputs,
        input_grad,
        norm_total[0],
        norm_total[1],
        stacked[0],
        grad_b_qkv,
        stacked[1],
        stacked[2],
        grad_b_one,
        stacked[3],
        norm_total[2],
    )


def solution(mesh):
    n_tensor = mesh.shape["tensor"]
    chips = mesh.shape["dp"] // 2
    fine = Mesh(mesh.devices.reshape(chips, 2, n_tensor), ("chip", "core", "tensor"))
    dp = ("chip", "core")
    every = ("chip", "core", "tensor")
    group = ("tensor", "chip", "core")
    in_specs = (
        P(every, None),
        P(every, None),
        P(None, dp),
        P(None, dp),
        P(None, dp, None, "tensor"),
        P(None, None, group),
        P(None, "tensor", dp),
        P(None, dp, "tensor"),
        P(None, group),
        P(None, "tensor", dp),
        P(None, dp),
    )
    out_specs = (
        P(every, None),
        P(every, None),
        P(None, every),
        P(None, every),
        P(None, dp, None, "tensor"),
        P(None, None, group),
        P(None, "tensor", dp),
        P(None, dp, "tensor"),
        P(None, group),
        P(None, "tensor", dp),
        P(None, every),
    )
    return jax.shard_map(
        functools.partial(on_device, chips, n_tensor), mesh=fine, in_specs=in_specs, out_specs=out_specs, check_vma=False
    )
```
